32 devices in a mesh: gx: 8 (over z, x), gy: 4 (over y, core).
Axes of the slice: x: 2, y: 2, z: 4, core: 2. Of those that a mesh axis runs over, the one named last changes fastest.
Arguments:
- displacement_old: float32 [3, 64, 64, 256], P(None, 'gx', 'gy'), may hold values from -6 to 6
- pressure_old: float32 [64, 64, 256], P('gx', 'gy'), may hold values from -6 to 6
- body_force: float32 [3, 64, 64, 256], P(None, 'gx', 'gy'), may hold values from -400 to 400
- fluid_source: float32 [64, 64, 256], P('gx', 'gy'), may hold values from -400 to 400
- material_ids: int32 [64, 64, 256], P('gx', 'gy'), may hold values from 0 to 7
- materials: float32 [5, 8], replicated, may hold values from 0.5 to 4
Outputs:
- displacement: float32 [3, 64, 64, 256], P(None, 'gx', 'gy')
- pressure: float32 [64, 64, 256], P('gx', 'gy')
The draws below stay inside these ranges and needn't reach their ends.
All inputs are finite; a program needn't handle non-finite values.
Results may differ from the reference program's by a relative error of at most 0.00017.
Values sent between devices are 32-bit elements; how exact they have to be, the bound alone decides.
A program may use at most 64 MiB of HBM per device.

```python
import math
import jax
import jax.numpy as jnp
from jax import lax

NZ = 256
NMAT = 8
OUTER = 2
INNER = 3
NX = 64
NY = 64


def field_scale(key):
    key_rise, key_across = jax.random.split(key)
    planes = jnp.arange(NX, dtype=jnp.float32) / NX
    rising = 10.0 ** planes * jnp.exp(jax.random.uniform(key_rise, (NX,), minval=-0.35, maxval=0.35))
    across = jnp.exp(jax.random.uniform(key_across, (NY,), minval=-1.2, maxval=1.2))
    return rising[:, None, None] * across[None, :, None]


def rough_field(key, shape):
    key_scale, key_values = jax.random.split(jax.random.fold_in(key, 17))
    scale = field_scale(key_scale)
    values = jnp.clip(jax.random.normal(key_values, shape, jnp.float32), -6.0, 6.0)
    return (values * scale).astype(jnp.float32)


def draw_body_force(key, part):
    return rough_field(jax.random.fold_in(key, 101), (3, NX, NY, NZ))


def draw_fluid_source(key, part):
    return rough_field(jax.random.fold_in(key, 202), (NX, NY, NZ))


def plant(values, stream_key, low, top_value):
    spot = [jax.random.randint(jax.random.fold_in(stream_key, axis), (), 0, length) for axis, length in enumerate(values.shape)]
    main_axis = values.shape.index(max(values.shape))
    beside = spot[:main_axis] + [(spot[main_axis] + 1) % values.shape[main_axis]] + spot[main_axis + 1:]
    return values.at[tuple(spot)].set(low).at[tuple(beside)].set(top_value)


def block_levels(rng, extent, pieces, least, largest):
    factor_of, own = 1.0, jax.random.fold_in(rng, 6)
    for axis_at, shards_of in pieces:
        draws = jnp.exp(jax.random.uniform(jax.random.fold_in(own, axis_at), (shards_of,), jnp.float32, least / len(pieces), largest / len(pieces)))
        factor_of = factor_of * jnp.repeat(draws, extent[axis_at] // shards_of).reshape([-1 if axis == axis_at else 1 for axis in range(len(extent))])
    return factor_of


def normal_values(own_key, dims, spread, limit, pieces=(), kind=jnp.bfloat16):
    gain = block_levels(own_key, dims, pieces, -0.22, 0.18) if pieces else 1.0
    result = jax.random.normal(own_key, dims, jnp.float32) * spread * gain
    return jnp.minimum(jnp.maximum(result, -limit), limit).astype(kind)


def setup_inputs(seed: int = 0) -> dict:
    keys = jax.random.split(jax.random.key(seed), 7)
    return {
        "displacement_old": normal_values(keys[0], (3, NX, NY, NZ), 1.0, 6.0, ((1, 8), (2, 4)), jnp.float32),
        "pressure_old": normal_values(keys[1], (NX, NY, NZ), 1.0, 6.0, ((0, 8), (1, 4)), jnp.float32),
        "body_force": draw_body_force(jax.random.fold_in(keys[6], 71), 0),
        "fluid_source": draw_fluid_source(jax.random.fold_in(keys[6], 71), 0),
        "material_ids": plant(jax.random.randint(keys[4], (NX, NY, NZ), 0, NMAT), jax.random.fold_in(keys[4], 1), 0, NMAT - 1).astype(jnp.int32),
        "materials": jnp.clip(jnp.exp(jax.random.uniform(keys[5], (5, NMAT), jnp.float32, math.log(0.5), math.log(4.0))), 0.5, 4.0),
    }


step_time = 4.0


def shift_up(values, spatial):
    length = values.shape[spatial]
    widths = [(0, 0)] * values.ndim
    widths[spatial] = (0, 1)
    return lax.slice_in_dim(jnp.pad(values, widths), 1, length + 1, axis=spatial)


def shift_down(values, spatial):
    length = values.shape[spatial]
    widths = [(0, 0)] * values.ndim
    widths[spatial] = (1, 0)
    return lax.slice_in_dim(jnp.pad(values, widths), 0, length, axis=spatial)


def harmonic(first_value, second_value):
    return 2.0 * first_value * second_value / (first_value + second_value)


def divergence(field):
    return (shift_up(field[0], 0) - field[0] + shift_up(field[1], 1) - field[1]
            + shift_up(field[2], 2) - field[2])


def solve(operate, precond, rhs_vec, initial):
    solution = initial
    residual = rhs_vec - operate(initial)
    smoothed = precond(residual)
    direction = smoothed
    current = jnp.sum(residual * smoothed)
    for inner_step in range(INNER):
        image_vec = operate(direction)
        step_length = current / jnp.sum(direction * image_vec)
        solution = solution + step_length * direction
        if inner_step + 1 < INNER:
            residual = residual - step_length * image_vec
            smoothed = precond(residual)
            following = jnp.sum(residual * smoothed)
            direction = smoothed + (following / current) * direction
            current = following
    return solution


def reference(displacement_old, pressure_old, body_force, fluid_source, material_ids, materials):
    lame_first = materials[0][material_ids]
    shear_mod = materials[1][material_ids]
    permeability = materials[2][material_ids]
    storage = materials[3][material_ids]
    biot_coef = 0.25 * materials[4][material_ids]
    stiff_up = [0.5 * (shear_mod + shift_up(shear_mod, spatial)) for spatial in range(3)]
    stiff_down = [0.5 * (shear_mod + shift_down(shear_mod, spatial)) for spatial in range(3)]
    flow_up = [harmonic(permeability, shift_up(permeability, spatial)) for spatial in range(3)]
    flow_down = [harmonic(permeability, shift_down(permeability, spatial)) for spatial in range(3)]
    stab = biot_coef * biot_coef / (lame_first + (2.0 / 3.0) * shear_mod)
    storage_total = storage + stab
    flow_sum = flow_up[0] + flow_down[0] + flow_up[1] + flow_down[1] + flow_up[2] + flow_down[2]
    inv_pressure = 1.0 / (storage_total + step_time * flow_sum)
    stiff_sum = stiff_up[0] + stiff_down[0] + stiff_up[1] + stiff_down[1] + stiff_up[2] + stiff_down[2]
    inv_blocks = 1.0 / jnp.stack([stiff_sum + shift_down(lame_first, spatial) for spatial in range(3)])
    factor = lame_first / (1.0 + lame_first * (inv_blocks[0] + inv_blocks[1] + inv_blocks[2]))

    def apply_pressure(field):
        flux = jnp.zeros_like(field)
        for spatial in range(3):
            flux = (flux + flow_up[spatial] * (field - shift_up(field, spatial))
                    + flow_down[spatial] * (field - shift_down(field, spatial)))
        return storage_total * field + step_time * flux

    def apply_mech(field):
        summed = jnp.zeros_like(field)
        for spatial in range(3):
            summed = (summed + stiff_up[spatial] * (field - shift_up(field, spatial + 1))
                      + stiff_down[spatial] * (field - shift_down(field, spatial + 1)))
        weighted = lame_first * divergence(field)
        lame_pull = jnp.stack([shift_down(weighted, spatial) - weighted for spatial in range(3)])
        return summed + lame_pull

    def solve_pressure(residual):
        return residual * inv_pressure

    def solve_blocks(residual):
        scaled = residual * inv_blocks
        summed = scaled[0] + scaled[1] + scaled[2]
        return scaled - inv_blocks * (factor * summed)

    pressure = pressure_old
    displacement = displacement_old
    for repeat in range(OUTER):
        change = displacement - displacement_old
        rhs_pressure = (storage * pressure_old + step_time * fluid_source
                        - biot_coef * divergence(change) + stab * pressure)
        pressure = solve(apply_pressure, solve_pressure, rhs_pressure, pressure)
        loaded = biot_coef * pressure
        pressure_push = jnp.stack([shift_down(loaded, spatial) - loaded for spatial in range(3)])
        rhs_mech = body_force + pressure_push
        displacement = solve(apply_mech, solve_blocks, rhs_mech, displacement)
    return displacement, pressure
```

```python
import functools
import jax
import jax.numpy as jnp
from jax import lax
from jax.experimental import pallas as pl
from jax.experimental.pallas import tpu as pltpu
from jax.sharding import PartitionSpec as P

OUTER = 2
INNER = 3
step_time = 4.0
MESH = pl.DeviceIdType.MESH
F32 = jnp.float32


def kernel(dims, *refs):
    ngx, ngy, nx, ny, nz, nmat = dims
    (mat, d_old, p_old, bforce, fsource, ids, d_out, p_out,
     XI, YIS, YIH, LAM, SHR, PRM, BIO, LAMY, SHRY, PRMY, BIOY, STO, STAB,
     SX, SY, SZ, SSUM, FX, FY, FZ, DIAG, PINV, HB, KF,
     PX, PYS, PYH, MX, MYS, MYH, MCS, MCH,
     WP, WM, RP, RM, AP, AD, DC, LY, RB1, RB2,
     isend, irecv, psend, precv, msend, mrecv, rsend1, rrecv1, rsend2, rrecv2) = refs
    gx, gy = lax.axis_index("gx"), lax.axis_index("gy")
    has = {(-1, 0): gx > 0, (1, 0): gx < ngx - 1, (0, -1): gy > 0, (0, 1): gy < ngy - 1}
    has[(1, -1)] = jnp.logical_and(has[(1, 0)], has[(0, -1)])
    has[(-1, 1)] = jnp.logical_and(has[(-1, 0)], has[(0, 1)])

    rows = lax.broadcasted_iota(jnp.int32, (ny, nz), 0)
    lanes = lax.broadcasted_iota(jnp.int32, (ny, nz), 1)
    lanes8 = lax.broadcasted_iota(jnp.int32, (nx, nz), 1)
    rows8 = lax.broadcasted_iota(jnp.int32, (nx, nz), 0)
    lane1 = lax.broadcasted_iota(jnp.int32, (1, 128), 1)
    first_row, last_row = rows == 0, rows == ny - 1
    first_lane, last_lane = lanes == 0, lanes == nz - 1
    zero = jnp.zeros((ny, nz), F32)
    zero8 = jnp.zeros((nx, nz), F32)

    def upz(v):
        return pltpu.roll(v, nz - 1, 1)

    def dnz(v):
        return pltpu.roll(v, 1, 1)

    def upy(v, halo):
        return jnp.where(last_row, halo, pltpu.roll(v, ny - 1, 0))

    def dny(v, halo):
        return jnp.where(first_row, halo, pltpu.roll(v, 1, 0))

    def fold(v):
        out = None
        for i in range(0, ny, 8):
            for j in range(0, nz, 128):
                part = v[i:i + 8, j:j + 128]
                out = part if out is None else out + part
        return out

    def loop(body, init, low=0, high=nx):
        return lax.fori_loop(low, high, body, init)

    def copies_of(pairs, send, recv):
        made = []
        for n, (src, dst, off) in enumerate(pairs):
            copy = pltpu.make_async_remote_copy(
                src_ref=src, dst_ref=dst, send_sem=send.at[n], recv_sem=recv.at[n],
                device_id=(gx + off[0], gy + off[1]), device_id_type=MESH)
            made.append((copy, off))
        return made

    def start(made):
        for copy, off in made:
            @pl.when(has[off])
            def _(copy=copy):
                copy.start()

    def wait_recv(made):
        for copy, off in made:
            @pl.when(has[(-off[0], -off[1])])
            def _(copy=copy):
                copy.wait_recv()

    def wait_send(made):
        for copy, off in made:
            @pl.when(has[off])
            def _(copy=copy):
                copy.wait_send()

    def scalar_field(f):
        return copies_of(
            [(PX.at[f, 1], PX.at[f, nx + 1], (-1, 0)), (PX.at[f, nx], PX.at[f, 0], (1, 0)),
             (PYS.at[f, 0], PYH.at[f, 1], (0, -1)), (PYS.at[f, 1], PYH.at[f, 0], (0, 1))],
            psend.at[f], precv.at[f])

    def vector_field(f):
        return copies_of(
            [(MX.at[f, :, 1], MX.at[f, :, nx + 1], (-1, 0)), (MX.at[f, :, nx], MX.at[f, :, 0], (1, 0)),
             (MYS.at[f, 0], MYH.at[f, 1], (0, -1)), (MYS.at[f, 1], MYH.at[f, 0], (0, 1)),
             (MCS.at[f, 0], MCH.at[f, 0], (1, -1)), (MCS.at[f, 1], MCH.at[f, 1], (-1, 1))],
            msend.at[f], mrecv.at[f])

    def put_scalar(f, i, v):
        PX[f, i + 1] = v
        PYS[f, 0, pl.ds(i, 1), :] = v[0:1]
        PYS[f, 1, pl.ds(i, 1), :] = v[ny - 1:ny]

    def put_vector(f, i, vs):
        for a in range(3):
            MX[f, a, i + 1] = vs[a]
            MYS[f, 0, a, pl.ds(i, 1), :] = vs[a][0:1]
            MYS[f, 1, a, pl.ds(i, 1), :] = vs[a][ny - 1:ny]

    def put_corners(f):
        MCS[f, 0] = MYS[f, 0, 1, nx - 1:nx, :]
        MCS[f, 1] = MYS[f, 1, 0, 0:1, :]

    nf = 1 + OUTER * INNER
    XI[0] = jnp.zeros((ny, nz), jnp.int32)
    XI[nx + 1] = jnp.zeros((ny, nz), jnp.int32)
    for s in range(2):
        YIH[s] = jnp.zeros((nx, nz), jnp.int32)

    def clear(f, c):
        PX[f, 0] = zero
        PX[f, nx + 1] = zero
        for s in range(2):
            PYH[f, s] = zero8
            MCH[f, s] = jnp.zeros((1, nz), F32)
            for a in range(3):
                MX[f, a, s * (nx + 1)] = zero
                MYH[f, s, a] = zero8
        return c
    lax.fori_loop(0, nf, clear, 0)

    barrier = pltpu.get_barrier_semaphore()
    for d in range(1, ngx):
        pl.semaphore_signal(barrier, inc=1, device_id=(lax.rem(gx + d, ngx), gy), device_id_type=MESH)
    for d in range(1, ngy):
        pl.semaphore_signal(barrier, inc=1, device_id=(gx, lax.rem(gy + d, ngy)), device_id_type=MESH)
    for off in ((1, -1), (-1, 1)):
        @pl.when(has[off])
        def _(off=off):
            pl.semaphore_signal(barrier, inc=1, device_id=(gx + off[0], gy + off[1]), device_id_type=MESH)

    def stage(i, c):
        code = ids[i] + 1
        XI[i + 1] = code
        YIS[0, pl.ds(i, 1), :] = code[0:1]
        YIS[1, pl.ds(i, 1), :] = code[ny - 1:ny]
        put_scalar(0, i, p_old[i])
        put_vector(0, i, [d_old[a, i] for a in range(3)])
        return c
    loop(stage, 0)
    put_corners(0)

    corners = has[(1, -1)].astype(jnp.int32) + has[(-1, 1)].astype(jnp.int32)
    pl.semaphore_wait(barrier, ngx - 1 + ngy - 1 + corners)

    codes_copy = copies_of(
        [(XI.at[1], XI.at[nx + 1], (-1, 0)), (XI.at[nx], XI.at[0], (1, 0)),
         (YIS.at[0], YIH.at[1], (0, -1)), (YIS.at[1], YIH.at[0], (0, 1))], isend, irecv)
    p_copy, d_copy = scalar_field(0), vector_field(0)
    start(codes_copy)
    start(p_copy)
    start(d_copy)

    def lookup(code, table_rows):
        out = [jnp.zeros(code.shape, F32) for _ in table_rows]
        for m in range(nmat):
            hit = code == m + 1
            out = [jnp.where(hit, mat[t, m], v) for t, v in zip(table_rows, out)]
        return out

    def look_plane(i, c):
        lam, shr, prm, sto, bio = lookup(XI[i + 1], (0, 1, 2, 3, 4))
        bio = 0.25 * bio
        LAM[i + 1] = lam
        SHR[i + 1] = shr
        PRM[i + 1] = prm
        BIO[i + 1] = bio
        STO[i] = sto
        STAB[i] = bio * bio / (lam + 2.0 / 3.0 * shr)
        return c
    loop(look_plane, 0)
    wait_recv(codes_copy)

    for j in (0, nx + 1):
        lam, shr, prm, bio = lookup(XI[j], (0, 1, 2, 4))
        LAM[j] = lam
        SHR[j] = shr
        PRM[j] = prm
        BIO[j] = 0.25 * bio
    for s in range(2):
        lam, shr, prm, bio = lookup(YIH[s], (0, 1, 2, 4))
        SHRY[s] = shr
        PRMY[s] = prm
        if s == 0:
            LAMY[...] = lam
            BIOY[...] = 0.25 * bio

    def harmonic(one, two):
        return (2.0 * step_time) * one * two / (one + two)

    def harmonic_plane(j, c):
        FX[j] = harmonic(PRM[j], PRM[j + 1])
        SX[j] = 0.5 * (SHR[j] + SHR[j + 1])
        return c
    loop(harmonic_plane, 0, 0, nx + 1)

    def coefs(i, c):
        shr, prm, lam = SHR[i + 1], PRM[i + 1], LAM[i + 1]
        row = pl.ds(i, 1)
        fyu = harmonic(prm, upy(prm, PRMY[1, row, :]))
        fyd = harmonic(prm, dny(prm, PRMY[0, row, :]))
        fzu = jnp.where(last_lane, 0.0, harmonic(prm, upz(prm)))
        fzd = jnp.where(first_lane, 0.0, dnz(fzu))
        FY[1, i], FY[0, i], FZ[1, i], FZ[0, i] = fyu, fyd, fzu, fzd
        diag = STO[i] + STAB[i] + (FX[i] + FX[i + 1] + fyu + fyd + fzu + fzd)
        DIAG[i] = diag
        PINV[i] = 1.0 / diag
        half = 0.5 * shr
        syu = 0.5 * (shr + upy(shr, SHRY[1, row, :]))
        syd = 0.5 * (shr + dny(shr, SHRY[0, row, :]))
        szu = half + jnp.where(last_lane, 0.0, 0.5 * upz(shr))
        szd = half + jnp.where(first_lane, 0.0, 0.5 * dnz(shr))
        total = SX[i] + SX[i + 1] + syu + syd + szu + szd
        SY[1, i], SY[0, i] = syu, syd
        SZ[1, i] = jnp.where(last_lane, 0.0, szu)
        SZ[0, i] = jnp.where(first_lane, 0.0, szd)
        SSUM[i] = total
        h0 = 1.0 / (total + LAM[i])
        h1 = 1.0 / (total + dny(lam, LAMY[row, :]))
        h2 = 1.0 / (total + jnp.where(first_lane, 0.0, dnz(lam)))
        HB[0, i], HB[1, i], HB[2, i] = h0, h1, h2
        KF[i] = lam / (1.0 + lam * (h0 + h1 + h2))
        return c
    loop(coefs, 0)

    def apply_pressure(f, emit, init):
        def body(i, c):
            row = pl.ds(i, 1)
            v = PX[f, i + 1]
            out = (DIAG[i] * v - FX[i + 1] * PX[f, i + 2] - FX[i] * PX[f, i]
                   - FY[1, i] * upy(v, PYH[f, 1, row, :]) - FY[0, i] * dny(v, PYH[f, 0, row, :])
                   - FZ[1, i] * upz(v) - FZ[0, i] * dnz(v))
            return emit(i, v, out, c)
        return loop(body, init)

    def apply_mech(f, emit, init):
        m = [MYH[f, 0, a] for a in range(3)]
        ahead = jnp.where(rows8 == nx - 1, MCH[f, 1], pltpu.roll(m[0], nx - 1, 0))
        z8 = jnp.where(lanes8 == nz - 1, 0.0, pltpu.roll(m[2], nz - 1, 1))
        LY[...] = LAMY[...] * (ahead - m[0] + MYS[f, 0, 1] - m[1] + z8 - m[2])
        m = [MX[f, a, 0] for a in range(3)]
        lprev = LAM[0] * (MX[f, 0, 1] - m[0] + upy(m[1], MCH[f, 0]) - m[1]
                          + jnp.where(last_lane, 0.0, upz(m[2])) - m[2])

        def body(i, carry):
            lprev, c = carry
            row = pl.ds(i, 1)
            ws, outs, div = [], [], None
            for a in range(3):
                w, wx = MX[f, a, i + 1], MX[f, a, i + 2]
                wy, wz = upy(w, MYH[f, 1, a, row, :]), upz(w)
                out = (SSUM[i] * w - SX[i + 1] * wx - SX[i] * MX[f, a, i]
                       - SY[1, i] * wy - SY[0, i] * dny(w, MYH[f, 0, a, row, :])
                       - SZ[1, i] * wz - SZ[0, i] * dnz(w))
                part = (wx, wy, jnp.where(last_lane, 0.0, wz))[a] - w
                div = part if div is None else div + part
                ws.append(w)
                outs.append(out)
            weighted = LAM[i + 1] * div
            below = (lprev, dny(weighted, LY[row, :]), jnp.where(first_lane, 0.0, dnz(weighted)))
            outs = [outs[a] + (below[a] - weighted) for a in range(3)]
            return weighted, emit(i, ws, outs, c)
        return loop(body, (lprev, init))[1]

    def block_solve(i, r):
        scaled = [r[a] * HB[a, i] for a in range(3)]
        tail = KF[i] * (scaled[0] + scaled[1] + scaled[2])
        return [scaled[a] - HB[a, i] * tail for a in range(3)]

    def dot3(a, b):
        return fold(a[0] * b[0] + a[1] * b[1] + a[2] * b[2])

    def all_sum(q, sums):
        row = jnp.zeros((1, 128), F32)
        for k, s in enumerate(sums):
            row = jnp.where(lane1 == k, jnp.sum(s, keepdims=True), row)
        for buf, send, recv, me, n, other in (
                (RB1, rsend1, rrecv1, gy, ngy, lambda t: (gx, t)),
                (RB2, rsend2, rrecv2, gx, ngx, lambda t: (t, gy))):
            buf[q, me] = row
            made = []
            for d in range(1, n):
                copy = pltpu.make_async_remote_copy(
                    src_ref=buf.at[q, me], dst_ref=buf.at[q, me], send_sem=send.at[q, d],
                    recv_sem=recv.at[q, d], device_id=other(lax.rem(me + d, n)), device_id_type=MESH)
                copy.start()
                made.append(copy)
            for copy in made:
                copy.wait_recv()
            for copy in made:
                copy.wait_send()
            row = buf[q, 0]
            for d in range(1, n):
                row = row + buf[q, d]
        return [row[:, k:k + 1] for k in range(len(sums))]

    def combine(t):
        n0, m0, m1, m2, m3, m4 = t
        n1 = m0 - n0
        n2 = m1 - n1
        l1, l2 = m1 / m0, m2 / m0
        d1 = m2 - l1 * m1
        e = m3 - l1 * m2
        l3 = jnp.where(d1 > 0, e / d1, 0.0)
        d2 = m4 - l2 * m2 - l3 * e
        y1 = n1 - l1 * n0
        y2 = n2 - l2 * n0 - l3 * y1
        c2 = jnp.where(d2 > 0, y2 / d2, 0.0)
        c1 = jnp.where(d1 > 0, y1 / d1, 0.0) - l3 * c2
        c0 = n0 / m0 - l1 * c1 - l2 * c2
        return c0, c1, c2

    zacc = jnp.zeros((8, 128), F32)
    wait_recv(p_copy)
    wait_send(p_copy)
    wait_send(codes_copy)

    def keep_ap(i, v, out, c):
        AP[i] = out
        return c
    apply_pressure(0, keep_ap, 0)

    def clear_change(i, c):
        DC[i] = zero
        for a in range(3):
            d_out[a, i] = d_old[a, i]
        return c
    loop(clear_change, 0)

    sent = []
    for outer in range(OUTER):
        base = 1 + INNER * outer

        def p_start(i, acc):
            rhs = (STO[i] * p_old[i] + step_time * fsource[i] - BIO[i + 1] * DC[i]
                   + STAB[i] * PX[0, i + 1])
            r = rhs - AP[i]
            u = r * PINV[i]
            put_scalar(base, i, u)
            return acc + fold(r * u)
        n0 = loop(p_start, zacc)
        made = scalar_field(base)
        start(made)
        sent.append(made)
        if outer == 0:
            wait_recv(d_copy)
            wait_send(d_copy)

            def keep_ad(i, ws, outs, c):
                for a in range(3):
                    AD[a, i] = outs[a]
                return c
            apply_mech(0, keep_ad, 0)
        sums = [n0]
        for k in range(INNER):
            wait_recv(made)

            def p_step(i, v, w, c):
                WP[k, i] = w
                even = c[0] + fold(v * w)
                if k == INNER - 1:
                    return (even,)
                u = w * PINV[i] - v
                put_scalar(base + k + 1, i, u)
                return even, c[1] + fold(u * w)
            sums += apply_pressure(base + k, p_step, (zacc,) * (1 if k == INNER - 1 else 2))
            if k < INNER - 1:
                made = scalar_field(base + k + 1)
                start(made)
                sent.append(made)
        cs = combine(all_sum(2 * outer, sums))

        def p_update(j, c):
            v = PX[0, j]
            for k in range(INNER):
                v = v + cs[k] * PX[base + k, j]
            PX[0, j] = v
            return c
        loop(p_update, 0, 0, nx + 1)
        ph = PYH[0, 0]
        for k in range(INNER):
            ph = ph + cs[k] * PYH[base + k, 0]
        PYH[0, 0] = ph
        LY[...] = BIOY[...] * ph

        def m_start(i, carry):
            before, acc = carry
            row = pl.ds(i, 1)
            load = BIO[i + 1] * PX[0, i + 1]
            below = (before, dny(load, LY[row, :]), jnp.where(first_lane, 0.0, dnz(load)))
            r = [bforce[a, i] + (below[a] - load) - AD[a, i] for a in range(3)]
            u = block_solve(i, r)
            put_vector(base, i, u)
            return load, acc + dot3(r, u)
        n0 = loop(m_start, (BIO[0] * PX[0, 0], zacc))[1]
        put_corners(base)
        made = vector_field(base)
        start(made)
        sent.append(made)

        def p_after(i, c):
            if outer == OUTER - 1:
                p_out[i] = PX[0, i + 1]
            else:
                v = AP[i]
                for k in range(INNER):
                    v = v + cs[k] * WP[k, i]
                AP[i] = v
            return c
        loop(p_after, 0)
        sums = [n0]
        for k in range(INNER):
            wait_recv(made)

            def m_step(i, v, w, c):
                if outer < OUTER - 1:
                    for a in range(3):
                        WM[k, a, i] = w[a]
                even = c[0] + dot3(v, w)
                if k == INNER - 1:
                    return (even,)
                z = block_solve(i, w)
                u = [z[a] - v[a] for a in range(3)]
                put_vector(base + k + 1, i, u)
                return even, c[1] + dot3(u, w)
            sums += apply_mech(base + k, m_step, (zacc,) * (1 if k == INNER - 1 else 2))
            if k < INNER - 1:
                put_corners(base + k + 1)
                made = vector_field(base + k + 1)
                start(made)
                sent.append(made)
        cs = combine(all_sum(2 * outer + 1, sums))

        def mixed(get):
            v = cs[0] * get(base)
            for k in range(1, INNER):
                v = v + cs[k] * get(base + k)
            return v

        def m_update(i, c):
            row = pl.ds(i, 1)
            change = [mixed(lambda f, a=a: MX[f, a, i + 1]) for a in range(3)]
            for a in range(3):
                d_out[a, i] = d_out[a, i] + change[a]
            if outer < OUTER - 1:
                for a in range(3):
                    v = AD[a, i]
                    for k in range(INNER):
                        v = v + cs[k] * WM[k, a, i]
                    AD[a, i] = v
                cx = mixed(lambda f: MX[f, 0, i + 2])
                cy = upy(change[1], mixed(lambda f: MYH[f, 1, 1, row, :]))
                cz = jnp.where(last_lane, 0.0, upz(change[2]))
                DC[i] = DC[i] + (cx - change[0] + cy - change[1] + cz - change[2])
            return c
        loop(m_update, 0)

    for made in sent:
        wait_send(made)


def on_device(dims, d_old, p_old, bforce, fsource, ids, materials):
    ngx, ngy, nx, ny, nz, nmat = dims
    nf = 1 + OUTER * INNER
    nq = 2 * OUTER

    def vm(*shape, dtype=F32):
        return pltpu.VMEM(shape, dtype)
    plane, strip = (ny, nz), (nx, nz)
    cell = (nx, ny, nz)
    ext = (nx + 2, ny, nz)
    dma = pltpu.SemaphoreType.DMA
    scratch = [
        vm(*ext, dtype=jnp.int32), vm(2, *strip, dtype=jnp.int32), vm(2, *strip, dtype=jnp.int32),
        vm(*ext), vm(*ext), vm(*ext), vm(*ext), vm(*strip), vm(2, *strip), vm(2, *strip), vm(*strip),
        vm(*cell), vm(*cell),
        vm(nx + 1, *plane), vm(2, *cell), vm(2, *cell), vm(*cell),
        vm(nx + 1, *plane), vm(2, *cell), vm(2, *cell), vm(*cell), vm(*cell),
        vm(3, *cell), vm(*cell),
        vm(nf, *ext), vm(nf, 2, *strip), vm(nf, 2, *strip),
        vm(nf, 3, *ext), vm(nf, 2, 3, *strip), vm(nf, 2, 3, *strip), vm(nf, 2, 1, nz), vm(nf, 2, 1, nz),
        vm(INNER, *cell), vm(INNER, 3, *cell), vm(8, 128), vm(8, 128), vm(*cell), vm(3, *cell), vm(*cell),
        vm(*strip), vm(nq, ngy, 1, 128), vm(nq, ngx, 1, 128),
        dma((4,)), dma((4,)), dma((nf, 4)), dma((nf, 4)), dma((nf, 6)), dma((nf, 6)),
        dma((nq, ngy)), dma((nq, ngy)), dma((nq, ngx)), dma((nq, ngx)),
    ]
    block = pl.BlockSpec(memory_space=pltpu.VMEM)
    return pl.pallas_call(
        functools.partial(kernel, dims),
        out_shape=(jax.ShapeDtypeStruct(d_old.shape, F32), jax.ShapeDtypeStruct(p_old.shape, F32)),
        in_specs=[pl.BlockSpec(memory_space=pltpu.SMEM)] + [block] * 5,
        out_specs=(block, block),
        scratch_shapes=scratch,
        compiler_params=pltpu.CompilerParams(
            collective_id=0, has_side_effects=True, vmem_limit_bytes=48 * 1024 * 1024),
        name="poro",
    )(materials, d_old, p_old, bforce, fsource, ids)


def solution(mesh):
    ngx, ngy = mesh.shape["gx"], mesh.shape["gy"]

    def body(d_old, p_old, bforce, fsource, ids, materials):
        dims = (ngx, ngy, *p_old.shape, materials.shape[1])
        return on_device(dims, d_old, p_old, bforce, fsource, ids, materials)

    return jax.shard_map(
        body,
        mesh=mesh,
        in_specs=(P(None, "gx", "gy", None), P("gx", "gy", None), P(None, "gx", "gy", None),
                  P("gx", "gy", None), P("gx", "gy", None), P()),
        out_specs=(P(None, "gx", "gy", None), P("gx", "gy", None)),
        check_vma=False,
    )
```

```python
import functools
import jax
import jax.numpy as jnp
from jax import lax
from jax.experimental import pallas as pl
from jax.experimental.pallas import tpu as pltpu
from jax.sharding import PartitionSpec as P

OUTER = 2
INNER = 3
step_time = 4.0
MESH = pl.DeviceIdType.MESH
F32 = jnp.float32


def kernel(dims, *refs):
    ngx, ngy, nx, ny, nz, nmat = dims
    (mat, d_hbm, p_hbm, bf_hbm, fs_hbm, ids_hbm, d_out, p_out,
     p_old, bforce, fsource, ids, lsem,
     XI, YIS, YIH, LAM, SHR, PRM, BIO, LAMY, SHRY, PRMY, BIOY, STO, STAB,
     SX, SY, SZ, SSUM, FX, FY, FZ, DIAG, PINV, HB, KF,
     PX, PYS, PYH, MX, MYS, MYH, MCS, MCH,
     WP, WM, AP, AD, DC, LY, LW, RB,
     isend, irecv, psend, precv, msend, mrecv, rsend, rrecv) = refs
    gx, gy = lax.axis_index("gx"), lax.axis_index("gy")
    has = {(-1, 0): gx > 0, (1, 0): gx < ngx - 1, (0, -1): gy > 0, (0, 1): gy < ngy - 1}
    has[(1, -1)] = jnp.logical_and(has[(1, 0)], has[(0, -1)])
    has[(-1, 1)] = jnp.logical_and(has[(-1, 0)], has[(0, 1)])

    rows = lax.broadcasted_iota(jnp.int32, (ny, nz), 0)
    lanes = lax.broadcasted_iota(jnp.int32, (ny, nz), 1)
    lanes8 = lax.broadcasted_iota(jnp.int32, (nx, nz), 1)
    rows8 = lax.broadcasted_iota(jnp.int32, (nx, nz), 0)
    lane1 = lax.broadcasted_iota(jnp.int32, (1, 128), 1)
    first_row, last_row = rows == 0, rows == ny - 1
    first_lane, last_lane = lanes == 0, lanes == nz - 1
    zero = jnp.zeros((ny, nz), F32)
    zero8 = jnp.zeros((nx, nz), F32)

    def upz(v):
        return pltpu.roll(v, nz - 1, 1)

    def dnz(v):
        return pltpu.roll(v, 1, 1)

    def upy(v, halo):
        return jnp.where(last_row, halo, pltpu.roll(v, ny - 1, 0))

    def dny(v, halo):
        return jnp.where(first_row, halo, pltpu.roll(v, 1, 0))

    def fold(v):
        out = None
        for i in range(0, ny, 8):
            for j in range(0, nz, 128):
                part = v[i:i + 8, j:j + 128]
                out = part if out is None else out + part
        return out

    def loop(body, init, low=0, high=nx, half=None):
        order = [low, high - 1] + list(range(low + 1, high - 1))
        for n, i in enumerate(order):
            init = body(i, init)
            if n == 1 and half is not None:
                half()
        return init

    def copies_of(pairs, send, recv):
        made = []
        for n, (src, dst, off) in enumerate(pairs):
            copy = pltpu.make_async_remote_copy(
                src_ref=src, dst_ref=dst, send_sem=send.at[n], recv_sem=recv.at[n],
                device_id=(gx + off[0], gy + off[1]), device_id_type=MESH)
            made.append((copy, off))
        return made

    def start(made, along=None):
        for copy, off in made:
            if along is not None and (off[0] != 0) != along:
                continue
            @pl.when(has[off])
            def _(copy=copy):
                copy.start()

    def wait_recv(made):
        for copy, off in made:
            @pl.when(has[(-off[0], -off[1])])
            def _(copy=copy):
                copy.wait_recv()

    def wait_send(made):
        for copy, off in made:
            @pl.when(has[off])
            def _(copy=copy):
                copy.wait_send()

    def scalar_field(f):
        return copies_of(
            [(PX.at[f, 1], PX.at[f, nx + 1], (-1, 0)), (PX.at[f, nx], PX.at[f, 0], (1, 0)),
             (PYS.at[f, 0], PYH.at[f, 1], (0, -1)), (PYS.at[f, 1], PYH.at[f, 0], (0, 1))],
            psend.at[f], precv.at[f])

    def vector_field(f):
        return copies_of(
            [(MX.at[f, :, 1], MX.at[f, :, nx + 1], (-1, 0)), (MX.at[f, :, nx], MX.at[f, :, 0], (1, 0)),
             (MYS.at[f, 0], MYH.at[f, 1], (0, -1)), (MYS.at[f, 1], MYH.at[f, 0], (0, 1)),
             (MCS.at[f, 0], MCH.at[f, 0], (1, -1)), (MCS.at[f, 1], MCH.at[f, 1], (-1, 1))],
            msend.at[f], mrecv.at[f])

    def put_scalar(f, i, v):
        PX[f, i + 1] = v
        PYS[f, 0, slice(i, i + 1), :] = v[0:1]
        PYS[f, 1, slice(i, i + 1), :] = v[ny - 1:ny]

    def put_vector(f, i, vs):
        for a in range(3):
            MX[f, a, i + 1] = vs[a]
            MYS[f, 0, a, slice(i, i + 1), :] = vs[a][0:1]
            MYS[f, 1, a, slice(i, i + 1), :] = vs[a][ny - 1:ny]

    def put_corners(f):
        MCS[f, 0] = MX[f, 1, nx, 0:1, :]
        MCS[f, 1] = MX[f, 0, 1, ny - 1:ny, :]

    local = [pltpu.make_async_copy(src, dst, lsem.at[n]) for n, (src, dst) in enumerate((
        (ids_hbm, ids), (p_hbm, PX.at[0, pl.ds(1, nx)]), (d_hbm, MX.at[0, :, pl.ds(1, nx)]),
        (p_hbm, p_old), (fs_hbm, fsource), (bf_hbm, bforce)))]
    for copy in local:
        copy.start()

    nf = 1 + OUTER * INNER
    XI[0] = jnp.zeros((ny, nz), jnp.int32)
    XI[nx + 1] = jnp.zeros((ny, nz), jnp.int32)
    for s in range(2):
        YIH[s] = jnp.zeros((nx, nz), jnp.int32)

    def clear(f, c):
        PX[f, 0] = zero
        PX[f, nx + 1] = zero
        for s in range(2):
            PYH[f, s] = zero8
            MCH[f, s] = jnp.zeros((1, nz), F32)
            for a in range(3):
                MX[f, a, s * (nx + 1)] = zero
                MYH[f, s, a] = zero8
        return c
    lax.fori_loop(0, nf, clear, 0)

    barrier = pltpu.get_barrier_semaphore()
    me, ndev = gx * ngy + gy, ngx * ngy

    def peer(d):
        t = lax.rem(me + d, ndev)
        return lax.div(t, ngy), lax.rem(t, ngy)
    for d in range(1, ndev):
        pl.semaphore_signal(barrier, inc=1, device_id=peer(d), device_id_type=MESH)

    def stage(i, c):
        code = ids[i] + 1
        XI[i + 1] = code
        YIS[0, slice(i, i + 1), :] = code[0:1]
        YIS[1, slice(i, i + 1), :] = code[ny - 1:ny]
        return c

    def stage_values(i, c):
        for side, y in ((0, 0), (1, ny - 1)):
            PYS[0, side, i:i + 1, :] = PX[0, i + 1, y:y + 1, :]
            for a in range(3):
                MYS[0, side, a, i:i + 1, :] = MX[0, a, i + 1, y:y + 1, :]
        return c
    local[0].wait()
    loop(stage, 0)
    local[1].wait()
    local[2].wait()
    loop(stage_values, 0)
    put_corners(0)
    pl.semaphore_wait(barrier, ndev - 1)

    codes_copy = copies_of(
        [(XI.at[1], XI.at[nx + 1], (-1, 0)), (XI.at[nx], XI.at[0], (1, 0)),
         (YIS.at[0], YIH.at[1], (0, -1)), (YIS.at[1], YIH.at[0], (0, 1))], isend, irecv)
    p_copy, d_copy = scalar_field(0), vector_field(0)
    start(codes_copy)
    start(p_copy)
    start(d_copy)

    def lookup(code, table_rows):
        out = [jnp.zeros(code.shape, F32) for _ in table_rows]
        for m in range(nmat):
            hit = code == m + 1
            out = [jnp.where(hit, mat[t, m], v) for t, v in zip(table_rows, out)]
        return out

    def look_plane(i, c):
        lam, shr, prm, sto, bio = lookup(XI[i + 1], (0, 1, 2, 3, 4))
        bio = 0.25 * bio
        LAM[i + 1] = lam
        SHR[i + 1] = shr
        PRM[i + 1] = prm
        BIO[i + 1] = bio
        STO[i] = sto
        STAB[i] = bio * bio / (lam + 2.0 / 3.0 * shr)
        return c
    loop(look_plane, 0)
    wait_recv(codes_copy)

    for j in (0, nx + 1):
        lam, shr, prm, bio = lookup(XI[j], (0, 1, 2, 4))
        LAM[j] = lam
        SHR[j] = shr
        PRM[j] = prm
        BIO[j] = 0.25 * bio
    for s in range(2):
        lam, shr, prm, bio = lookup(YIH[s], (0, 1, 2, 4))
        SHRY[s] = shr
        PRMY[s] = prm
        if s == 0:
            LAMY[...] = lam
            BIOY[...] = 0.25 * bio

    def harmonic(one, two):
        return (2.0 * step_time) * one * two / (one + two)

    def harmonic_plane(j, c):
        FX[j] = harmonic(PRM[j], PRM[j + 1])
        SX[j] = 0.5 * (SHR[j] + SHR[j + 1])
        return c
    loop(harmonic_plane, 0, 0, nx + 1)

    def coefs(i, c):
        shr, prm, lam = SHR[i + 1], PRM[i + 1], LAM[i + 1]
        row = slice(i, i + 1)
        fyu = harmonic(prm, upy(prm, PRMY[1, row, :]))
        fyd = harmonic(prm, dny(prm, PRMY[0, row, :]))
        fzu = jnp.where(last_lane, 0.0, harmonic(prm, upz(prm)))
        fzd = jnp.where(first_lane, 0.0, dnz(fzu))
        FY[1, i], FY[0, i], FZ[1, i], FZ[0, i] = fyu, fyd, fzu, fzd
        diag = STO[i] + STAB[i] + (FX[i] + FX[i + 1] + fyu + fyd + fzu + fzd)
        DIAG[i] = diag
        PINV[i] = 1.0 / diag
        half = 0.5 * shr
        syu = 0.5 * (shr + upy(shr, SHRY[1, row, :]))
        syd = 0.5 * (shr + dny(shr, SHRY[0, row, :]))
        szu = half + jnp.where(last_lane, 0.0, 0.5 * upz(shr))
        szd = half + jnp.where(first_lane, 0.0, 0.5 * dnz(shr))
        total = SX[i] + SX[i + 1] + syu + syd + szu + szd
        SY[1, i], SY[0, i] = syu, syd
        SZ[1, i] = jnp.where(last_lane, 0.0, szu)
        SZ[0, i] = jnp.where(first_lane, 0.0, szd)
        SSUM[i] = total
        h0 = 1.0 / (total + LAM[i])
        h1 = 1.0 / (total + dny(lam, LAMY[row, :]))
        h2 = 1.0 / (total + jnp.where(first_lane, 0.0, dnz(lam)))
        HB[0, i], HB[1, i], HB[2, i] = h0, h1, h2
        KF[i] = lam / (1.0 + lam * (h0 + h1 + h2))
        return c
    loop(coefs, 0)

    def apply_pressure(f, emit, init, half=None):
        def body(i, c):
            row = slice(i, i + 1)
            v = PX[f, i + 1]
            out = (DIAG[i] * v - FX[i + 1] * PX[f, i + 2] - FX[i] * PX[f, i]
                   - FY[1, i] * upy(v, PYH[f, 1, row, :]) - FY[0, i] * dny(v, PYH[f, 0, row, :])
                   - FZ[1, i] * upz(v) - FZ[0, i] * dnz(v))
            return emit(i, v, out, c)
        return loop(body, init, half=half)

    def apply_mech(f, emit, init, half=None):
        m = [MYH[f, 0, a] for a in range(3)]
        ahead = jnp.where(rows8 == nx - 1, MCH[f, 1], pltpu.roll(m[0], nx - 1, 0))
        z8 = jnp.where(lanes8 == nz - 1, 0.0, pltpu.roll(m[2], nz - 1, 1))
        LY[...] = LAMY[...] * (ahead - m[0] + MYS[f, 0, 1] - m[1] + z8 - m[2])
        m = [MX[f, a, 0] for a in range(3)]
        below_first = LAM[0] * (MX[f, 0, 1] - m[0] + upy(m[1], MCH[f, 0]) - m[1]
                          + jnp.where(last_lane, 0.0, upz(m[2])) - m[2])

        def weigh(i):
            w = [MX[f, a, i + 1] for a in range(3)]
            return LAM[i + 1] * (MX[f, 0, i + 2] - w[0] + upy(w[1], MYH[f, 1, 1, i:i + 1, :]) - w[1]
                                 + jnp.where(last_lane, 0.0, upz(w[2])) - w[2])

        def body(i, c):
            row = slice(i, i + 1)
            ws, outs, div = [], [], None
            for a in range(3):
                w, wx = MX[f, a, i + 1], MX[f, a, i + 2]
                wy, wz = upy(w, MYH[f, 1, a, row, :]), upz(w)
                out = (SSUM[i] * w - SX[i + 1] * wx - SX[i] * MX[f, a, i]
                       - SY[1, i] * wy - SY[0, i] * dny(w, MYH[f, 0, a, row, :])
                       - SZ[1, i] * wz - SZ[0, i] * dnz(w))
                part = (wx, wy, jnp.where(last_lane, 0.0, wz))[a] - w
                div = part if div is None else div + part
                ws.append(w)
                outs.append(out)
            weighted = LAM[i + 1] * div
            LW[i] = weighted
            before = below_first if i == 0 else weigh(i - 1) if i == nx - 1 else LW[i - 1]
            below = (before, dny(weighted, LY[row, :]), jnp.where(first_lane, 0.0, dnz(weighted)))
            outs = [outs[a] + (below[a] - weighted) for a in range(3)]
            return emit(i, ws, outs, c)
        return loop(body, init, half=half)

    def block_solve(i, r):
        scaled = [r[a] * HB[a, i] for a in range(3)]
        tail = KF[i] * (scaled[0] + scaled[1] + scaled[2])
        return [scaled[a] - HB[a, i] * tail for a in range(3)]

    def dot3(a, b):
        return fold(a[0] * b[0] + a[1] * b[1] + a[2] * b[2])

    summed = []

    def all_sum(q, sums):
        row = jnp.zeros((1, 128), F32)
        for k, s in enumerate(sums):
            row = jnp.where(lane1 == k, jnp.sum(s, keepdims=True), row)
        RB[q, me] = row
        made = []
        for d in range(1, ndev):
            copy = pltpu.make_async_remote_copy(
                src_ref=RB.at[q, me], dst_ref=RB.at[q, me], send_sem=rsend.at[q, d],
                recv_sem=rrecv.at[q, d], device_id=peer(d), device_id_type=MESH)
            copy.start()
            made.append(copy)
        for copy in made:
            copy.wait_recv()
        summed.extend(made)
        parts = [RB[q, d] for d in range(ndev)]
        while len(parts) > 1:
            parts = [sum(parts[d + 1:d + 2], parts[d]) for d in range(0, len(parts), 2)]
        row = parts[0]
        return [row[:, k:k + 1] for k in range(len(sums))]

    def combine(t):
        n0, m0, m1, m2, m3, m4 = t
        n1 = m0 - n0
        n2 = m1 - n1
        l1, l2 = m1 / m0, m2 / m0
        d1 = m2 - l1 * m1
        e = m3 - l1 * m2
        l3 = jnp.where(d1 > 0, e / d1, 0.0)
        d2 = m4 - l2 * m2 - l3 * e
        y1 = n1 - l1 * n0
        y2 = n2 - l2 * n0 - l3 * y1
        c2 = jnp.where(d2 > 0, y2 / d2, 0.0)
        c1 = jnp.where(d1 > 0, y1 / d1, 0.0) - l3 * c2
        c0 = n0 / m0 - l1 * c1 - l2 * c2
        return c0, c1, c2

    zacc = jnp.zeros((8, 128), F32)
    wait_recv(p_copy)
    wait_send(p_copy)
    wait_send(codes_copy)

    def keep_ap(i, v, out, c):
        AP[i] = out
        return c
    apply_pressure(0, keep_ap, 0)

    def clear_change(i, c):
        DC[i] = zero
        return c
    loop(clear_change, 0)
    local[3].wait()
    local[4].wait()

    sent = []
    for outer in range(OUTER):
        base = 1 + INNER * outer

        def p_start(i, acc):
            rhs = (STO[i] * p_old[i] + step_time * fsource[i] - BIO[i + 1] * DC[i]
                   + STAB[i] * PX[0, i + 1])
            r = rhs - AP[i]
            u = r * PINV[i]
            put_scalar(base, i, u)
            return acc + fold(r * u)
        made = scalar_field(base)
        n0 = loop(p_start, zacc, half=functools.partial(start, made, True))
        start(made, False)
        sent.append(made)
        if outer > 0:
            loop(m_after, 0)
        if outer == 0:
            wait_recv(d_copy)
            wait_send(d_copy)

            def keep_ad(i, ws, outs, c):
                for a in range(3):
                    AD[a, i] = outs[a]
                return c
            apply_mech(0, keep_ad, 0)
            local[5].wait()
        sums = [n0]
        for k in range(INNER):
            wait_recv(made)

            def p_step(i, v, w, c):
                WP[k, i] = w
                even = c[0] + fold(v * w)
                if k == INNER - 1:
                    return (even,)
                u = w * PINV[i] - v
                put_scalar(base + k + 1, i, u)
                return even, c[1] + fold(u * w)
            half = None
            if k < INNER - 1:
                made = scalar_field(base + k + 1)
                half = functools.partial(start, made, True)
            sums += apply_pressure(base + k, p_step, (zacc,) * (1 if k == INNER - 1 else 2), half)
            if k < INNER - 1:
                start(made, False)
                sent.append(made)
        cs = combine(all_sum(2 * outer, sums))

        def p_update(j, c):
            v = PX[0, j]
            for k in range(INNER):
                v = v + cs[k] * PX[base + k, j]
            PX[0, j] = v
            return c
        loop(p_update, 0, 0, nx + 1)
        ph = PYH[0, 0]
        for k in range(INNER):
            ph = ph + cs[k] * PYH[base + k, 0]
        PYH[0, 0] = ph
        LY[...] = BIOY[...] * ph

        def m_start(i, acc):
            row = slice(i, i + 1)
            load = BIO[i + 1] * PX[0, i + 1]
            below = (BIO[i] * PX[0, i], dny(load, LY[row, :]), jnp.where(first_lane, 0.0, dnz(load)))
            r = [bforce[a, i] + (below[a] - load) - AD[a, i] for a in range(3)]
            u = block_solve(i, r)
            put_vector(base, i, u)
            return acc + dot3(r, u)
        made = vector_field(base)

        def send_planes(f, made):
            put_corners(f)
            start(made, True)
        n0 = loop(m_start, zacc, half=functools.partial(send_planes, base, made))
        start(made, False)
        sent.append(made)

        def p_after(i, c):
            if outer == OUTER - 1:
                p_out[i] = PX[0, i + 1]
            else:
                v = AP[i]
                for k in range(INNER):
                    v = v + cs[k] * WP[k, i]
                AP[i] = v
            return c
        loop(p_after, 0)
        sums = [n0]
        for k in range(INNER):
            wait_recv(made)

            def m_step(i, v, w, c):
                if outer < OUTER - 1:
                    for a in range(3):
                        WM[k, a, i] = w[a]
                even = c[0] + dot3(v, w)
                if k == INNER - 1:
                    return (even,)
                z = block_solve(i, w)
                u = [z[a] - v[a] for a in range(3)]
                put_vector(base + k + 1, i, u)
                return even, c[1] + dot3(u, w)
            half = None
            if k < INNER - 1:
                made = vector_field(base + k + 1)
                half = functools.partial(send_planes, base + k + 1, made)
            sums += apply_mech(base + k, m_step, (zacc,) * (1 if k == INNER - 1 else 2), half)
            if k < INNER - 1:
                start(made, False)
                sent.append(made)
        cs = combine(all_sum(2 * outer + 1, sums))

        def mixed(get, cs=cs, base=base):
            v = cs[0] * get(base)
            for k in range(1, INNER):
                v = v + cs[k] * get(base + k)
            return v

        def m_change(i, c):
            row = slice(i, i + 1)
            change = [mixed(lambda f, a=a: MX[f, a, i + 1]) for a in range(3)]
            cx = mixed(lambda f: MX[f, 0, i + 2])
            cy = upy(change[1], mixed(lambda f: MYH[f, 1, 1, row, :]))
            cz = jnp.where(last_lane, 0.0, upz(change[2]))
            DC[i] = DC[i] + (cx - change[0] + cy - change[1] + cz - change[2])
            return c

        def m_after(i, c, cs=cs, mixed=mixed, outer=outer):
            for a in range(3):
                before = MX[0, a, i + 1] if outer == 0 else d_out[a, i]
                d_out[a, i] = before + mixed(lambda f, a=a: MX[f, a, i + 1])
            if outer < OUTER - 1:
                for a in range(3):
                    v = AD[a, i]
                    for k in range(INNER):
                        v = v + cs[k] * WM[k, a, i]
                    AD[a, i] = v
            return c
        loop(m_change if outer < OUTER - 1 else m_after, 0)

    for made in sent:
        wait_send(made)
    for copy in summed:
        copy.wait_send()


def on_device(dims, d_old, p_old, bforce, fsource, ids, materials):
    ngx, ngy, nx, ny, nz, nmat = dims
    nf = 1 + OUTER * INNER
    nq = 2 * OUTER

    def vm(*shape, dtype=F32):
        return pltpu.VMEM(shape, dtype)
    plane, strip = (ny, nz), (nx, nz)
    cell = (nx, ny, nz)
    ext = (nx + 2, ny, nz)
    dma = pltpu.SemaphoreType.DMA
    scratch = [
        vm(*cell), vm(3, *cell), vm(*cell), vm(*cell, dtype=jnp.int32), dma((6,)),
        vm(*ext, dtype=jnp.int32), vm(2, *strip, dtype=jnp.int32), vm(2, *strip, dtype=jnp.int32),
        vm(*ext), vm(*ext), vm(*ext), vm(*ext), vm(*strip), vm(2, *strip), vm(2, *strip), vm(*strip),
        vm(*cell), vm(*cell),
        vm(nx + 1, *plane), vm(2, *cell), vm(2, *cell), vm(*cell),
        vm(nx + 1, *plane), vm(2, *cell), vm(2, *cell), vm(*cell), vm(*cell),
        vm(3, *cell), vm(*cell),
        vm(nf, *ext), vm(nf, 2, *strip), vm(nf, 2, *strip),
        vm(nf, 3, *ext), vm(nf, 2, 3, *strip), vm(nf, 2, 3, *strip), vm(nf, 2, 1, nz), vm(nf, 2, 1, nz),
        vm(INNER, *cell), vm(INNER, 3, *cell), vm(*cell), vm(3, *cell), vm(*cell),
        vm(*strip), vm(*cell), vm(nq, ngx * ngy, 1, 128),
        dma((4,)), dma((4,)), dma((nf, 4)), dma((nf, 4)), dma((nf, 6)), dma((nf, 6)),
        dma((nq, ngx * ngy)), dma((nq, ngx * ngy)),
    ]
    block = pl.BlockSpec(memory_space=pltpu.VMEM)
    return pl.pallas_call(
        functools.partial(kernel, dims),
        out_shape=(jax.ShapeDtypeStruct(d_old.shape, F32), jax.ShapeDtypeStruct(p_old.shape, F32)),
        in_specs=[pl.BlockSpec(memory_space=pltpu.SMEM)] + [pl.BlockSpec(memory_space=pl.ANY)] * 5,
        out_specs=(block, block),
        scratch_shapes=scratch,
        compiler_params=pltpu.CompilerParams(
            collective_id=0, has_side_effects=True, vmem_limit_bytes=63 * 1024 * 1024),
        name="poro",
    )(materials, d_old, p_old, bforce, fsource, ids)


def solution(mesh):
    ngx, ngy = mesh.shape["gx"], mesh.shape["gy"]

    def body(d_old, p_old, bforce, fsource, ids, materials):
        dims = (ngx, ngy, *p_old.shape, materials.shape[1])
        return on_device(dims, d_old, p_old, bforce, fsource, ids, materials)

    return jax.shard_map(
        body,
        mesh=mesh,
        in_specs=(P(None, "gx", "gy", None), P("gx", "gy", None), P(None, "gx", "gy", None),
                  P("gx", "gy", None), P("gx", "gy", None), P()),
        out_specs=(P(None, "gx", "gy", None), P("gx", "gy", None)),
        check_vma=False,
    )
```

```python
import functools
import jax
import jax.numpy as jnp
from jax import lax
from jax.experimental import pallas as pl
from jax.experimental.pallas import tpu as pltpu
from jax.sharding import PartitionSpec as P

OUTER = 2
INNER = 3
step_time = 4.0
MESH = pl.DeviceIdType.MESH
F32 = jnp.float32


def kernel(dims, *refs):
    ngx, ngy, nx, ny, nz, nmat = dims
    (mat, d_hbm, p_hbm, bf_hbm, fs_hbm, ids_hbm, d_out, p_out,
     p_old, bforce, fsource, ids, lsem,
     XI, YIS, YIH, LAM, SHR, PRM, BIO, LAMY, SHRY, PRMY, BIOY, STO, STAB,
     SX, SY, SZ, SSUM, FX, FY, FZ, DIAG, PINV, HB, KF,
     PX, PYS, PYH, MX, MYS, MYH, MCS, MCH,
     WP, WM, AP, AD, DC, LY, LW, RB,
     isend, irecv, psend, precv, msend, mrecv, rsend, rrecv) = refs
    gx, gy = lax.axis_index("gx"), lax.axis_index("gy")
    has = {(-1, 0): gx > 0, (1, 0): gx < ngx - 1, (0, -1): gy > 0, (0, 1): gy < ngy - 1}
    has[(1, -1)] = jnp.logical_and(has[(1, 0)], has[(0, -1)])
    has[(-1, 1)] = jnp.logical_and(has[(-1, 0)], has[(0, 1)])

    rows = lax.broadcasted_iota(jnp.int32, (ny, nz), 0)
    lanes = lax.broadcasted_iota(jnp.int32, (ny, nz), 1)
    lanes8 = lax.broadcasted_iota(jnp.int32, (nx, nz), 1)
    rows8 = lax.broadcasted_iota(jnp.int32, (nx, nz), 0)
    lane1 = lax.broadcasted_iota(jnp.int32, (1, 128), 1)
    first_row, last_row = rows == 0, rows == ny - 1
    first_lane, last_lane = lanes == 0, lanes == nz - 1
    zero = jnp.zeros((ny, nz), F32)
    zero8 = jnp.zeros((nx, nz), F32)

    def upz(v):
        return pltpu.roll(v, nz - 1, 1)

    def dnz(v):
        return pltpu.roll(v, 1, 1)

    def upy(v, halo):
        return jnp.where(last_row, halo, pltpu.roll(v, ny - 1, 0))

    def dny(v, halo):
        return jnp.where(first_row, halo, pltpu.roll(v, 1, 0))

    def fold(v):
        out = None
        for i in range(0, ny, 8):
            for j in range(0, nz, 128):
                part = v[i:i + 8, j:j + 128]
                out = part if out is None else out + part
        return out

    def loop(body, init, low=0, high=nx, half=None):
        order = [low, high - 1] + list(range(low + 1, high - 1))
        for n, i in enumerate(order):
            init = body(i, init)
            if n == 1 and half is not None:
                half()
        return init

    def copies_of(pairs, send, recv):
        made = []
        for n, (src, dst, off) in enumerate(pairs):
            copy = pltpu.make_async_remote_copy(
                src_ref=src, dst_ref=dst, send_sem=send.at[n], recv_sem=recv.at[n],
                device_id=(gx + off[0], gy + off[1]), device_id_type=MESH)
            made.append((copy, off))
        return made

    def start(made, along=None):
        for copy, off in made:
            if along is not None and (off[0] != 0) != along:
                continue
            @pl.when(has[off])
            def _(copy=copy):
                copy.start()

    def wait_recv(made):
        for copy, off in made:
            @pl.when(has[(-off[0], -off[1])])
            def _(copy=copy):
                copy.wait_recv()

    def wait_send(made):
        for copy, off in made:
            @pl.when(has[off])
            def _(copy=copy):
                copy.wait_send()

    def scalar_field(f):
        return copies_of(
            [(PX.at[f, 1], PX.at[f, nx + 1], (-1, 0)), (PX.at[f, nx], PX.at[f, 0], (1, 0)),
             (PYS.at[f, 0], PYH.at[f, 1], (0, -1)), (PYS.at[f, 1], PYH.at[f, 0], (0, 1))],
            psend.at[f], precv.at[f])

    def vector_field(f):
        return copies_of(
            [(MX.at[f, :, 1], MX.at[f, :, nx + 1], (-1, 0)), (MX.at[f, :, nx], MX.at[f, :, 0], (1, 0)),
             (MYS.at[f, 0], MYH.at[f, 1], (0, -1)), (MYS.at[f, 1], MYH.at[f, 0], (0, 1)),
             (MCS.at[f, 0], MCH.at[f, 0], (1, -1)), (MCS.at[f, 1], MCH.at[f, 1], (-1, 1))],
            msend.at[f], mrecv.at[f])

    def put_scalar(f, i, v):
        PX[f, i + 1] = v
        PYS[f, 0, slice(i, i + 1), :] = v[0:1]
        PYS[f, 1, slice(i, i + 1), :] = v[ny - 1:ny]

    def put_vector(f, i, vs):
        for a in range(3):
            MX[f, a, i + 1] = vs[a]
            MYS[f, 0, a, slice(i, i + 1), :] = vs[a][0:1]
            MYS[f, 1, a, slice(i, i + 1), :] = vs[a][ny - 1:ny]

    def put_corners(f):
        MCS[f, 0] = MX[f, 1, nx, 0:1, :]
        MCS[f, 1] = MX[f, 0, 1, ny - 1:ny, :]

    local = [pltpu.make_async_copy(src, dst, lsem.at[n]) for n, (src, dst) in enumerate((
        (ids_hbm, ids), (p_hbm, PX.at[0, pl.ds(1, nx)]), (d_hbm, MX.at[0, :, pl.ds(1, nx)]),
        (p_hbm, p_old), (fs_hbm, fsource), (bf_hbm, bforce)))]
    for copy in local:
        copy.start()

    nf = 1 + OUTER * INNER
    XI[0] = jnp.zeros((ny, nz), jnp.int32)
    XI[nx + 1] = jnp.zeros((ny, nz), jnp.int32)
    for s in range(2):
        YIH[s] = jnp.zeros((nx, nz), jnp.int32)

    def clear(f, c):
        PX[f, 0] = zero
        PX[f, nx + 1] = zero
        for s in range(2):
            PYH[f, s] = zero8
            MCH[f, s] = jnp.zeros((1, nz), F32)
            for a in range(3):
                MX[f, a, s * (nx + 1)] = zero
                MYH[f, s, a] = zero8
        return c
    lax.fori_loop(0, nf, clear, 0)

    barrier = pltpu.get_barrier_semaphore()
    me, ndev = gx * ngy + gy, ngx * ngy

    def peer(d):
        t = lax.rem(me + d, ndev)
        return lax.div(t, ngy), lax.rem(t, ngy)
    for d in range(1, ndev):
        pl.semaphore_signal(barrier, inc=1, device_id=peer(d), device_id_type=MESH)

    def stage(i, c):
        code = ids[i] + 1
        XI[i + 1] = code
        YIS[0, slice(i, i + 1), :] = code[0:1]
        YIS[1, slice(i, i + 1), :] = code[ny - 1:ny]
        return c

    def stage_values(i, c):
        for side, y in ((0, 0), (1, ny - 1)):
            PYS[0, side, i:i + 1, :] = PX[0, i + 1, y:y + 1, :]
            for a in range(3):
                MYS[0, side, a, i:i + 1, :] = MX[0, a, i + 1, y:y + 1, :]
        return c
    local[0].wait()
    loop(stage, 0)
    local[1].wait()
    local[2].wait()
    loop(stage_values, 0)
    put_corners(0)
    pl.semaphore_wait(barrier, ndev - 1)

    codes_copy = copies_of(
        [(XI.at[1], XI.at[nx + 1], (-1, 0)), (XI.at[nx], XI.at[0], (1, 0)),
         (YIS.at[0], YIH.at[1], (0, -1)), (YIS.at[1], YIH.at[0], (0, 1))], isend, irecv)
    p_copy, d_copy = scalar_field(0), vector_field(0)
    start(codes_copy)
    start(p_copy)
    start(d_copy)

    def lookup(code, table_rows):
        out = [jnp.zeros(code.shape, F32) for _ in table_rows]
        for m in range(nmat):
            hit = code == m + 1
            out = [jnp.where(hit, mat[t, m], v) for t, v in zip(table_rows, out)]
        return out

    def look_plane(i, c):
        lam, shr, prm, sto, bio = lookup(XI[i + 1], (0, 1, 2, 3, 4))
        bio = 0.25 * bio
        LAM[i + 1] = lam
        SHR[i + 1] = shr
        PRM[i + 1] = prm
        BIO[i + 1] = bio
        STO[i] = sto
        STAB[i] = bio * bio / (lam + 2.0 / 3.0 * shr)
        return c
    loop(look_plane, 0)
    wait_recv(codes_copy)

    for j in (0, nx + 1):
        lam, shr, prm, bio = lookup(XI[j], (0, 1, 2, 4))
        LAM[j] = lam
        SHR[j] = shr
        PRM[j] = prm
        BIO[j] = 0.25 * bio
    for s in range(2):
        lam, shr, prm, bio = lookup(YIH[s], (0, 1, 2, 4))
        SHRY[s] = shr
        PRMY[s] = prm
        if s == 0:
            LAMY[...] = lam
            BIOY[...] = 0.25 * bio

    def harmonic(one, two):
        return (2.0 * step_time) * one * two / (one + two)

    def harmonic_plane(j, c):
        FX[j] = harmonic(PRM[j], PRM[j + 1])
        SX[j] = 0.5 * (SHR[j] + SHR[j + 1])
        return c
    loop(harmonic_plane, 0, 0, nx + 1)

    def coefs(i, c):
        shr, prm, lam = SHR[i + 1], PRM[i + 1], LAM[i + 1]
        row = slice(i, i + 1)
        fyu = harmonic(prm, upy(prm, PRMY[1, row, :]))
        fyd = harmonic(prm, dny(prm, PRMY[0, row, :]))
        fzu = jnp.where(last_lane, 0.0, harmonic(prm, upz(prm)))
        fzd = jnp.where(first_lane, 0.0, dnz(fzu))
        FY[1, i], FY[0, i], FZ[1, i], FZ[0, i] = fyu, fyd, fzu, fzd
        diag = STO[i] + STAB[i] + (FX[i] + FX[i + 1] + fyu + fyd + fzu + fzd)
        DIAG[i] = diag
        PINV[i] = 1.0 / diag
        half = 0.5 * shr
        syu = 0.5 * (shr + upy(shr, SHRY[1, row, :]))
        syd = 0.5 * (shr + dny(shr, SHRY[0, row, :]))
        szu = half + jnp.where(last_lane, 0.0, 0.5 * upz(shr))
        szd = half + jnp.where(first_lane, 0.0, 0.5 * dnz(shr))
        total = SX[i] + SX[i + 1] + syu + syd + szu + szd
        SY[1, i], SY[0, i] = syu, syd
        SZ[1, i] = jnp.where(last_lane, 0.0, szu)
        SZ[0, i] = jnp.where(first_lane, 0.0, szd)
        SSUM[i] = total
        h0 = 1.0 / (total + LAM[i])
        h1 = 1.0 / (total + dny(lam, LAMY[row, :]))
        h2 = 1.0 / (total + jnp.where(first_lane, 0.0, dnz(lam)))
        HB[0, i], HB[1, i], HB[2, i] = h0, h1, h2
        KF[i] = lam / (1.0 + lam * (h0 + h1 + h2))
        return c
    loop(coefs, 0)

    def apply_pressure(f, emit, init, half=None):
        def body(i, c):
            row = slice(i, i + 1)
            v = PX[f, i + 1]
            out = (DIAG[i] * v - FX[i + 1] * PX[f, i + 2] - FX[i] * PX[f, i]
                   - FY[1, i] * upy(v, PYH[f, 1, row, :]) - FY[0, i] * dny(v, PYH[f, 0, row, :])
                   - FZ[1, i] * upz(v) - FZ[0, i] * dnz(v))
            return emit(i, v, out, c)
        return loop(body, init, half=half)

    def apply_mech(f, emit, init, half=None):
        m = [MYH[f, 0, a] for a in range(3)]
        ahead = jnp.where(rows8 == nx - 1, MCH[f, 1], pltpu.roll(m[0], nx - 1, 0))
        z8 = jnp.where(lanes8 == nz - 1, 0.0, pltpu.roll(m[2], nz - 1, 1))
        LY[...] = LAMY[...] * (ahead - m[0] + MYS[f, 0, 1] - m[1] + z8 - m[2])
        m = [MX[f, a, 0] for a in range(3)]
        below_first = LAM[0] * (MX[f, 0, 1] - m[0] + upy(m[1], MCH[f, 0]) - m[1]
                          + jnp.where(last_lane, 0.0, upz(m[2])) - m[2])

        def weigh(i):
            w = [MX[f, a, i + 1] for a in range(3)]
            return LAM[i + 1] * (MX[f, 0, i + 2] - w[0] + upy(w[1], MYH[f, 1, 1, i:i + 1, :]) - w[1]
                                 + jnp.where(last_lane, 0.0, upz(w[2])) - w[2])

        def body(i, c):
            row = slice(i, i + 1)
            ws, outs, div = [], [], None
            for a in range(3):
                w, wx = MX[f, a, i + 1], MX[f, a, i + 2]
                wy, wz = upy(w, MYH[f, 1, a, row, :]), upz(w)
                out = (SSUM[i] * w - SX[i + 1] * wx - SX[i] * MX[f, a, i]
                       - SY[1, i] * wy - SY[0, i] * dny(w, MYH[f, 0, a, row, :])
                       - SZ[1, i] * wz - SZ[0, i] * dnz(w))
                part = (wx, wy, jnp.where(last_lane, 0.0, wz))[a] - w
                div = part if div is None else div + part
                ws.append(w)
                outs.append(out)
            weighted = LAM[i + 1] * div
            LW[i] = weighted
            before = below_first if i == 0 else weigh(i - 1) if i == nx - 1 else LW[i - 1]
            below = (before, dny(weighted, LY[row, :]), jnp.where(first_lane, 0.0, dnz(weighted)))
            outs = [outs[a] + (below[a] - weighted) for a in range(3)]
            return emit(i, ws, outs, c)
        return loop(body, init, half=half)

    def block_solve(i, r):
        scaled = [r[a] * HB[a, i] for a in range(3)]
        tail = KF[i] * (scaled[0] + scaled[1] + scaled[2])
        return [scaled[a] - HB[a, i] * tail for a in range(3)]

    def dot3(a, b):
        return fold(a[0] * b[0] + a[1] * b[1] + a[2] * b[2])

    summed = []

    def all_sum(q, sums):
        row = jnp.zeros((1, 128), F32)
        for k, s in enumerate(sums):
            row = jnp.where(lane1 == k, jnp.sum(s, keepdims=True), row)
        RB[q, me] = row
        made = []
        for d in sorted(range(1, ndev), key=lambda d: -min(d, ndev - d)):
            copy = pltpu.make_async_remote_copy(
                src_ref=RB.at[q, me], dst_ref=RB.at[q, me], send_sem=rsend.at[q, d],
                recv_sem=rrecv.at[q, d], device_id=peer(d), device_id_type=MESH)
            copy.start()
            made.append(copy)
        for copy in made:
            copy.wait_recv()
        summed.extend(made)
        parts = [RB[q, d] for d in range(ndev)]
        while len(parts) > 1:
            parts = [sum(parts[d + 1:d + 2], parts[d]) for d in range(0, len(parts), 2)]
        row = parts[0]
        return [row[:, k:k + 1] for k in range(len(sums))]

    def combine(t):
        n0, m0, m1, m2, m3, m4 = t
        n1 = m0 - n0
        n2 = m1 - n1
        l1, l2 = m1 / m0, m2 / m0
        d1 = m2 - l1 * m1
        e = m3 - l1 * m2
        l3 = jnp.where(d1 > 0, e / d1, 0.0)
        d2 = m4 - l2 * m2 - l3 * e
        y1 = n1 - l1 * n0
        y2 = n2 - l2 * n0 - l3 * y1
        c2 = jnp.where(d2 > 0, y2 / d2, 0.0)
        c1 = jnp.where(d1 > 0, y1 / d1, 0.0) - l3 * c2
        c0 = n0 / m0 - l1 * c1 - l2 * c2
        return c0, c1, c2

    zacc = jnp.zeros((8, 128), F32)
    wait_recv(p_copy)
    wait_send(p_copy)
    wait_send(codes_copy)

    def keep_ap(i, v, out, c):
        AP[i] = out
        return c
    apply_pressure(0, keep_ap, 0)

    def clear_change(i, c):
        DC[i] = zero
        return c
    loop(clear_change, 0)
    local[3].wait()
    local[4].wait()

    sent = []
    for outer in range(OUTER):
        base = 1 + INNER * outer

        def p_start(i, acc):
            if outer > 0:
                m_change(i, 0)
            rhs = (STO[i] * p_old[i] + step_time * fsource[i] - BIO[i + 1] * DC[i]
                   + STAB[i] * PX[0, i + 1])
            r = rhs - AP[i]
            u = r * PINV[i]
            put_scalar(base, i, u)
            return acc + fold(r * u)
        made = scalar_field(base)
        n0 = loop(p_start, zacc, half=functools.partial(start, made, True))
        start(made, False)
        sent.append(made)
        if outer > 0:
            loop(m_after, 0)
        if outer == 0:
            wait_recv(d_copy)
            wait_send(d_copy)

            def keep_ad(i, ws, outs, c):
                for a in range(3):
                    AD[a, i] = outs[a]
                return c
            apply_mech(0, keep_ad, 0)
            local[5].wait()
        sums = [n0]
        for k in range(INNER):
            sums = [jnp.sum(v, keepdims=True) for v in sums]
            wait_recv(made)

            def p_step(i, v, w, c):
                WP[k, i] = w
                even = c[0] + fold(v * w)
                if k == INNER - 1:
                    return (even,)
                u = w * PINV[i] - v
                put_scalar(base + k + 1, i, u)
                return even, c[1] + fold(u * w)
            half = None
            if k < INNER - 1:
                made = scalar_field(base + k + 1)
                half = functools.partial(start, made, True)
            sums += apply_pressure(base + k, p_step, (zacc,) * (1 if k == INNER - 1 else 2), half)
            if k < INNER - 1:
                start(made, False)
                sent.append(made)
        cs = combine(all_sum(2 * outer, sums))

        def p_update(j, c):
            v = PX[0, j]
            for k in range(INNER):
                v = v + cs[k] * PX[base + k, j]
            PX[0, j] = v
            return c
        loop(p_update, 0, 0, nx + 1)
        ph = PYH[0, 0]
        for k in range(INNER):
            ph = ph + cs[k] * PYH[base + k, 0]
        PYH[0, 0] = ph
        LY[...] = BIOY[...] * ph

        def m_start(i, acc):
            row = slice(i, i + 1)
            load = BIO[i + 1] * PX[0, i + 1]
            below = (BIO[i] * PX[0, i], dny(load, LY[row, :]), jnp.where(first_lane, 0.0, dnz(load)))
            r = [bforce[a, i] + (below[a] - load) - AD[a, i] for a in range(3)]
            u = block_solve(i, r)
            put_vector(base, i, u)
            return acc + dot3(r, u)
        made = vector_field(base)

        def send_planes(f, made):
            put_corners(f)
            start(made, True)
        n0 = loop(m_start, zacc, half=functools.partial(send_planes, base, made))
        start(made, False)
        sent.append(made)

        def p_after(i, c):
            if outer == OUTER - 1:
                p_out[i] = PX[0, i + 1]
            else:
                v = AP[i]
                for k in range(INNER):
                    v = v + cs[k] * WP[k, i]
                AP[i] = v
            return c
        loop(p_after, 0)
        sums = [n0]
        for k in range(INNER):
            sums = [jnp.sum(v, keepdims=True) for v in sums]
            wait_recv(made)

            def m_step(i, v, w, c):
                if outer < OUTER - 1:
                    for a in range(3):
                        WM[k, a, i] = w[a]
                even = c[0] + dot3(v, w)
                if k == INNER - 1:
                    return (even,)
                z = block_solve(i, w)
                u = [z[a] - v[a] for a in range(3)]
                put_vector(base + k + 1, i, u)
                return even, c[1] + dot3(u, w)
            half = None
            if k < INNER - 1:
                made = vector_field(base + k + 1)
                half = functools.partial(send_planes, base + k + 1, made)
            sums += apply_mech(base + k, m_step, (zacc,) * (1 if k == INNER - 1 else 2), half)
            if k < INNER - 1:
                start(made, False)
                sent.append(made)
        cs = combine(all_sum(2 * outer + 1, sums))

        def mixed(get, cs=cs, base=base):
            v = cs[0] * get(base)
            for k in range(1, INNER):
                v = v + cs[k] * get(base + k)
            return v

        def m_change(i, c):
            row = slice(i, i + 1)
            change = [mixed(lambda f, a=a: MX[f, a, i + 1]) for a in range(3)]
            cx = mixed(lambda f: MX[f, 0, i + 2])
            cy = upy(change[1], mixed(lambda f: MYH[f, 1, 1, row, :]))
            cz = jnp.where(last_lane, 0.0, upz(change[2]))
            DC[i] = DC[i] + (cx - change[0] + cy - change[1] + cz - change[2])
            return c

        def m_after(i, c, cs=cs, mixed=mixed, outer=outer):
            for a in range(3):
                before = MX[0, a, i + 1] if outer == 0 else d_out[a, i]
                d_out[a, i] = before + mixed(lambda f, a=a: MX[f, a, i + 1])
            if outer < OUTER - 1:
                for a in range(3):
                    v = AD[a, i]
                    for k in range(INNER):
                        v = v + cs[k] * WM[k, a, i]
                    AD[a, i] = v
            return c
        if outer == OUTER - 1:
            loop(m_after, 0)

    for made in sent:
        wait_send(made)
    for copy in summed:
        copy.wait_send()


def on_device(dims, d_old, p_old, bforce, fsource, ids, materials):
    ngx, ngy, nx, ny, nz, nmat = dims
    nf = 1 + OUTER * INNER
    nq = 2 * OUTER

    def vm(*shape, dtype=F32):
        return pltpu.VMEM(shape, dtype)
    plane, strip = (ny, nz), (nx, nz)
    cell = (nx, ny, nz)
    ext = (nx + 2, ny, nz)
    dma = pltpu.SemaphoreType.DMA
    scratch = [
        vm(*cell), vm(3, *cell), vm(*cell), vm(*cell, dtype=jnp.int32), dma((6,)),
        vm(*ext, dtype=jnp.int32), vm(2, *strip, dtype=jnp.int32), vm(2, *strip, dtype=jnp.int32),
        vm(*ext), vm(*ext), vm(*ext), vm(*ext), vm(*strip), vm(2, *strip), vm(2, *strip), vm(*strip),
        vm(*cell), vm(*cell),
        vm(nx + 1, *plane), vm(2, *cell), vm(2, *cell), vm(*cell),
        vm(nx + 1, *plane), vm(2, *cell), vm(2, *cell), vm(*cell), vm(*cell),
        vm(3, *cell), vm(*cell),
        vm(nf, *ext), vm(nf, 2, *strip), vm(nf, 2, *strip),
        vm(nf, 3, *ext), vm(nf, 2, 3, *strip), vm(nf, 2, 3, *strip), vm(nf, 2, 1, nz), vm(nf, 2, 1, nz),
        vm(INNER, *cell), vm(INNER, 3, *cell), vm(*cell), vm(3, *cell), vm(*cell),
        vm(*strip), vm(*cell), vm(nq, ngx * ngy, 1, 128),
        dma((4,)), dma((4,)), dma((nf, 4)), dma((nf, 4)), dma((nf, 6)), dma((nf, 6)),
        dma((nq, ngx * ngy)), dma((nq, ngx * ngy)),
    ]
    block = pl.BlockSpec(memory_space=pltpu.VMEM)
    return pl.pallas_call(
        functools.partial(kernel, dims),
        out_shape=(jax.ShapeDtypeStruct(d_old.shape, F32), jax.ShapeDtypeStruct(p_old.shape, F32)),
        in_specs=[pl.BlockSpec(memory_space=pltpu.SMEM)] + [pl.BlockSpec(memory_space=pl.ANY)] * 5,
        out_specs=(block, block),
        scratch_shapes=scratch,
        compiler_params=pltpu.CompilerParams(
            collective_id=0, has_side_effects=True, vmem_limit_bytes=63 * 1024 * 1024),
        name="poro",
    )(materials, d_old, p_old, bforce, fsource, ids)


def solution(mesh):
    ngx, ngy = mesh.shape["gx"], mesh.shape["gy"]

    def body(d_old, p_old, bforce, fsource, ids, materials):
        dims = (ngx, ngy, *p_old.shape, materials.shape[1])
        return on_device(dims, d_old, p_old, bforce, fsource, ids, materials)

    return jax.shard_map(
        body,
        mesh=mesh,
        in_specs=(P(None, "gx", "gy", None), P("gx", "gy", None), P(None, "gx", "gy", None),
                  P("gx", "gy", None), P("gx", "gy", None), P()),
        out_specs=(P(None, "gx", "gy", None), P("gx", "gy", None)),
        check_vma=False,
    )
```
